8 devices in a mesh: dp: 1 (over z), sp: 8 (over y, x, core).
Axes of the slice: x: 2, y: 2, z: 1, core: 2. Of those that a mesh axis runs over, the one named last changes fastest.
Arguments:
- tokens: bfloat16 [16, 2048, 4096], P('dp', 'sp')
- w_query: bfloat16 [4096, 4096], replicated
- w_key: bfloat16 [4096, 1024], replicated
- w_value: bfloat16 [4096, 1024], replicated
- w_out: bfloat16 [4096, 4096], replicated
- attn_norm: bfloat16 [4096], replicated
- q_norm: bfloat16 [128], replicated
- k_norm: bfloat16 [128], replicated
Outputs:
- output 1: bfloat16 [16, 2048, 4096], P('dp', 'sp')
- output 2: bfloat16 [16, 2048, 8, 128], P('dp', 'sp')
- output 3: bfloat16 [16, 2048, 8, 128], P('dp', 'sp')
All inputs are finite; a program needn't handle non-finite values.
Results may differ from the reference program's by a relative error of at most 0.00828378.
Values are sent between devices in bfloat16 or wider.
A program may use at most 1 GiB of HBM per device.

```python
import jax
import jax.numpy as jnp
from jax import lax

BATCH = 16
SEQ_LEN = 2048
D_MODEL = 4096
HEADS = 32
KV_HEADS = 8
HEAD_DIM = 128
EPS = 1e-6
THETA = 1000000.0
Q_BLOCK = min(128, SEQ_LEN)
N_QBLK = SEQ_LEN // Q_BLOCK
GROUP = HEADS // KV_HEADS
SCALE = HEAD_DIM ** -0.5


def rms_norm(values, gain_vec):
    wide_vals = values.astype(jnp.float32)
    inv_rms = lax.rsqrt(jnp.mean(wide_vals * wide_vals, axis=-1, keepdims=True) + EPS)
    return wide_vals * inv_rms * gain_vec.astype(jnp.float32)


def rope_rotate(values, positions):
    half_dim = HEAD_DIM // 2
    inv_freq = THETA ** (-jnp.arange(half_dim, dtype=jnp.float32) * 2.0 / HEAD_DIM)
    angles = positions.astype(jnp.float32)[:, None] * inv_freq[None, :]
    cos_t = jnp.cos(angles)[None, :, None, :]
    sin_t = jnp.sin(angles)[None, :, None, :]
    lo_half = values[..., :half_dim]
    hi_half = values[..., half_dim:]
    return jnp.concatenate([lo_half * cos_t - hi_half * sin_t, hi_half * cos_t + lo_half * sin_t], axis=-1)


def setup_inputs(seed: int = 0, part: int = 0) -> dict:
    part_key = jax.random.fold_in(jax.random.key(seed), part)
    noise_key, walk_key = jax.random.split(part_key, 2)
    shared = jax.random.split(jax.random.key(seed + 1), 7)
    noise_part = 0.5 * jax.random.normal(noise_key, (BATCH, SEQ_LEN, D_MODEL), jnp.float32)
    walk_steps = jax.random.normal(walk_key, (BATCH, SEQ_LEN, D_MODEL), jnp.float32)
    walk_part = jnp.cumsum(walk_steps, axis=1) * (1.5 / SEQ_LEN ** 0.5)
    tokens = (noise_part + walk_part).astype(jnp.bfloat16)

    def make_dense(rng_key, fan_in, fan_out):
        return (jax.random.normal(rng_key, (fan_in, fan_out), jnp.float32) * fan_in ** -0.5).astype(jnp.bfloat16)

    def draw_gain(rng_key, n_elems, center, spread):
        return (center + spread * jax.random.normal(rng_key, (n_elems,), jnp.float32)).astype(jnp.bfloat16)

    return {
        'tokens': tokens,
        'w_query': make_dense(shared[0], D_MODEL, HEADS * HEAD_DIM),
        'w_key': make_dense(shared[1], D_MODEL, KV_HEADS * HEAD_DIM),
        'w_value': make_dense(shared[2], D_MODEL, KV_HEADS * HEAD_DIM),
        'w_out': make_dense(shared[3], HEADS * HEAD_DIM, D_MODEL),
        'attn_norm': draw_gain(shared[4], D_MODEL, 1.0, 0.3),
        'q_norm': draw_gain(shared[5], HEAD_DIM, 1.4, 0.4),
        'k_norm': draw_gain(shared[6], HEAD_DIM, 1.4, 0.4),
    }


def reference(tokens, w_query, w_key, w_value, w_out, attn_norm, q_norm, k_norm):
    hidden = rms_norm(tokens, attn_norm).astype(jnp.bfloat16).reshape(BATCH * SEQ_LEN, D_MODEL)
    q_proj = jnp.dot(hidden, w_query, preferred_element_type=jnp.float32).astype(jnp.bfloat16).reshape(BATCH, SEQ_LEN, HEADS, HEAD_DIM)
    k_proj = jnp.dot(hidden, w_key, preferred_element_type=jnp.float32).astype(jnp.bfloat16).reshape(BATCH, SEQ_LEN, KV_HEADS, HEAD_DIM)
    v_proj = jnp.dot(hidden, w_value, preferred_element_type=jnp.float32).astype(jnp.bfloat16).reshape(BATCH, SEQ_LEN, KV_HEADS, HEAD_DIM)
    positions = jnp.arange(SEQ_LEN)
    q_rot = rope_rotate(rms_norm(q_proj, q_norm), positions).astype(jnp.bfloat16)
    k_rot = rope_rotate(rms_norm(k_proj, k_norm), positions).astype(jnp.bfloat16)
    key_pos = jnp.arange(SEQ_LEN)
    row_ids = jnp.arange(Q_BLOCK)

    def one_seq(seq_args):
        q_seq, k_seq, v_seq = seq_args
        k_wide = k_seq.astype(jnp.float32)
        v_wide = v_seq.astype(jnp.float32)
        q_blocks = q_seq.reshape(N_QBLK, Q_BLOCK, KV_HEADS, GROUP, HEAD_DIM)

        def one_block(blk_args):
            q_blk, blk_idx = blk_args
            scores = jnp.einsum('qkgd,skd->kgqs', q_blk.astype(jnp.float32), k_wide) * SCALE
            allowed = key_pos[None, :] <= (blk_idx * Q_BLOCK + row_ids)[:, None]
            scores = jnp.where(allowed[None, None], scores, -jnp.inf)
            probs_blk = jax.nn.softmax(scores, axis=-1)
            return jnp.einsum('kgqs,skd->qkgd', probs_blk, v_wide).astype(jnp.bfloat16)

        attn_blocks = lax.map(one_block, (q_blocks, jnp.arange(N_QBLK)))
        return attn_blocks.reshape(SEQ_LEN, HEADS * HEAD_DIM)

    attn_out = lax.map(one_seq, (q_rot, k_rot, v_proj))
    proj_out = jnp.dot(attn_out.reshape(BATCH * SEQ_LEN, HEADS * HEAD_DIM), w_out, preferred_element_type=jnp.float32)
    output = (tokens.astype(jnp.float32) + proj_out.reshape(BATCH, SEQ_LEN, D_MODEL)).astype(jnp.bfloat16)
    return (output, k_rot, v_proj)
```

```python
import functools

import jax
import jax.numpy as jnp
from jax import lax
from jax.experimental import pallas as pl
from jax.experimental.pallas import tpu as pltpu
from jax.sharding import PartitionSpec as P

EPS = 1e-6
THETA = 1000000.0
HD = 128
LOG2E = 1.4426950408889634
VMEM_LIMIT = 60 * 1024 * 1024


def rope_tables(positions):
    half = HD // 2
    inv_freq = THETA ** (-jnp.arange(half, dtype=jnp.float32) * 2.0 / HD)
    angles = positions.astype(jnp.float32)[:, None] * inv_freq[None, :]
    cos_t, sin_t = jnp.cos(angles), jnp.sin(angles)
    return jnp.concatenate([cos_t, cos_t], axis=1), jnp.concatenate([-sin_t, sin_t], axis=1)


def head_norm_rope(raw, gain, cos_t, sin_t):
    inv = lax.rsqrt(jnp.mean(raw * raw, axis=-1, keepdims=True) + EPS)
    normed = raw * inv * gain
    return normed * cos_t + pltpu.roll(normed, HD // 2, 1) * sin_t


def kv_kernel(x_ref, g_ref, wk_ref, wv_ref, kg_ref, cos_ref, sin_ref, h_ref, kv_ref):
    wide = x_ref[...].astype(jnp.float32)
    inv = lax.rsqrt(jnp.mean(wide * wide, axis=-1, keepdims=True) + EPS)
    h_ref[...] = (wide * inv * g_ref[...]).astype(jnp.bfloat16)
    hid = h_ref[...]
    n_k = wk_ref.shape[1]
    step = 512
    for c in range(0, n_k, step):
        raw = jnp.dot(hid, wk_ref[:, c:c + step], preferred_element_type=jnp.float32)
        raw = raw.astype(jnp.bfloat16).astype(jnp.float32)
        for j in range(0, step, HD):
            k_rot = head_norm_rope(raw[:, j:j + HD], kg_ref[...], cos_ref[...], sin_ref[...])
            kv_ref[:, c + j:c + j + HD] = k_rot.astype(jnp.bfloat16)
    for c in range(0, n_k, step):
        raw = jnp.dot(hid, wv_ref[:, c:c + step], preferred_element_type=jnp.float32)
        kv_ref[:, n_k + c:n_k + c + step] = raw.astype(jnp.bfloat16)


def kv_project(x, w_key, w_value, attn_gain, k_gain, cos_t, sin_t):
    rows, d_model = x.shape
    n_k = w_key.shape[1]
    tok = cos_t.shape[0]
    bm = 256
    rep = tok // bm
    tab = pl.BlockSpec((bm, HD), lambda i: (i % rep, 0))
    full = lambda a: pl.BlockSpec(a.shape, lambda i: (0, 0), pipeline_mode=pl.Buffered(1))
    return pl.pallas_call(
        kv_kernel,
        grid=(rows // bm,),
        in_specs=[pl.BlockSpec((bm, d_model), lambda i: (i, 0)), full(attn_gain), full(w_key), full(w_value), full(k_gain), tab, tab],
        out_specs=[pl.BlockSpec((bm, d_model), lambda i: (i, 0)), pl.BlockSpec((bm, 2 * n_k), lambda i: (i, 0))],
        out_shape=[jax.ShapeDtypeStruct((rows, d_model), jnp.bfloat16), jax.ShapeDtypeStruct((rows, 2 * n_k), jnp.bfloat16)],
        compiler_params=pltpu.CompilerParams(vmem_limit_bytes=VMEM_LIMIT, dimension_semantics=('arbitrary',)),
        cost_estimate=pl.CostEstimate(flops=2 * rows * d_model * 2 * n_k, bytes_accessed=rows * d_model * 4 + 4 * d_model * n_k, transcendentals=0),
        name='kv_project',
    )(x, attn_gain, w_key, w_value, k_gain, cos_t, sin_t)


def attn_kernel(n_group, blk, idx_ref, q_ref, k_ref, v_ref, qg_ref, cos_ref, sin_ref, o_ref, q_s, acc_s, m_s, l_s):
    idx = idx_ref[0]
    scale = LOG2E * HD ** -0.5
    for h in range(n_group):
        raw = q_ref[:, h * HD:(h + 1) * HD].astype(jnp.float32)
        q_s[h] = head_norm_rope(raw, qg_ref[...], cos_ref[...], sin_ref[...]).astype(jnp.bfloat16)

    def fold(p):
        part = p[:, :HD]
        for j in range(HD, p.shape[1], HD):
            part = part + p[:, j:j + HD]
        return part

    def scores(h, k_blk):
        return lax.dot_general(q_s[h], k_blk, (((1,), (1,)), ((), ())), preferred_element_type=jnp.float32) * scale

    def first(start, n_blk):
        k_blk = k_ref[pl.ds(start, n_blk)].reshape(n_blk * blk, HD)
        v_blk = v_ref[pl.ds(start, n_blk)].reshape(n_blk * blk, HD)
        shape = (blk, n_blk * blk)
        allowed = lax.broadcasted_iota(jnp.int32, shape, 1) <= lax.broadcasted_iota(jnp.int32, shape, 0) + (n_blk - 1) * blk
        for h in range(n_group):
            s = jnp.where(allowed, scores(h, k_blk), -jnp.inf)
            m = jnp.broadcast_to(jnp.max(s, axis=1, keepdims=True), (blk, HD))
            p = jnp.exp2(s - jnp.concatenate([m] * (shape[1] // HD), axis=1))
            m_s[h] = m
            l_s[h] = fold(p)
            acc_s[h] = jnp.dot(p.astype(jnp.bfloat16), v_blk, preferred_element_type=jnp.float32)

    pl.when(idx % 2 == 0)(lambda: first(idx, 1))
    pl.when(idx % 2 == 1)(lambda: first(idx - 1, 2))

    def body(j, _):
        k_blk = k_ref[pl.ds(2 * j, 2)].reshape(2 * blk, HD)
        v_blk = v_ref[pl.ds(2 * j, 2)].reshape(2 * blk, HD)
        for h in range(n_group):
            s = scores(h, k_blk)
            m_old = m_s[h]
            m = jnp.maximum(m_old, jnp.broadcast_to(jnp.max(s, axis=1, keepdims=True), (blk, HD)))
            alpha = jnp.exp2(m_old - m)
            p = jnp.exp2(s - jnp.concatenate([m] * (2 * blk // HD), axis=1))
            m_s[h] = m
            l_s[h] = l_s[h] * alpha + fold(p)
            acc_s[h] = acc_s[h] * alpha + jnp.dot(p.astype(jnp.bfloat16), v_blk, preferred_element_type=jnp.float32)
        return 0

    lax.fori_loop(0, idx // 2, body, 0)
    for h in range(n_group):
        total = jnp.sum(l_s[h], axis=1, keepdims=True)
        o_ref[:, h * HD:(h + 1) * HD] = (acc_s[h] * (1.0 / total)).astype(jnp.bfloat16)


def attention(idx, q, kv_all, q_gain, cos_t, sin_t):
    n_dev, rows, kv_w = kv_all.shape
    n_kv = kv_w // (2 * HD)
    n_group = q.shape[1] // (n_kv * HD)
    blk = cos_t.shape[0]
    n_b = rows // blk
    tab = pl.BlockSpec((blk, HD), lambda b, h, i: (0, 0))
    qo = pl.BlockSpec((blk, n_group * HD), lambda b, h, i: (b, h))
    flops = 4 * rows * q.shape[1] * n_dev * blk * 2
    return pl.pallas_call(
        functools.partial(attn_kernel, n_group, blk),
        grid_spec=pltpu.PrefetchScalarGridSpec(
            num_scalar_prefetch=1,
            grid=(n_b, n_kv),
            in_specs=[qo, pl.BlockSpec((n_dev, blk, HD), lambda b, h, i: (0, b, h)), pl.BlockSpec((n_dev, blk, HD), lambda b, h, i: (0, b, n_kv + h)), pl.BlockSpec((1, HD), lambda b, h, i: (0, 0)), tab, tab],
            out_specs=qo,
            scratch_shapes=[pltpu.VMEM((n_group, blk, HD), jnp.bfloat16)] + [pltpu.VMEM((n_group, blk, HD), jnp.float32)] * 3,
        ),
        out_shape=jax.ShapeDtypeStruct(q.shape, jnp.bfloat16),
        compiler_params=pltpu.CompilerParams(vmem_limit_bytes=VMEM_LIMIT, dimension_semantics=('arbitrary', 'arbitrary')),
        cost_estimate=pl.CostEstimate(flops=flops, bytes_accessed=4 * rows * q.shape[1] + 2 * kv_all.size, transcendentals=0),
        name='attention',
    )(idx, q, kv_all, kv_all, q_gain, cos_t, sin_t)


def solution(mesh):
    def per_device(tokens, w_query, w_key, w_value, w_out, attn_norm, q_norm, k_norm):
        n_batch, seq_loc, d_model = tokens.shape
        me = lax.axis_index('sp')
        cos_t, sin_t = rope_tables(me * seq_loc + jnp.arange(seq_loc))
        attn_gain = attn_norm.astype(jnp.float32)[None, :]
        q_gain = q_norm.astype(jnp.float32)[None, :]
        k_gain = k_norm.astype(jnp.float32)[None, :]
        idx = jnp.reshape(me, (1,)).astype(jnp.int32)
        flat = tokens.reshape(n_batch * seq_loc, d_model)
        n_kv = w_key.shape[1] // HD

        n_chunk = 4
        rows = n_batch * seq_loc // n_chunk
        parts = [flat[g * rows:(g + 1) * rows] for g in range(n_chunk)]
        hid, kv, kv_all = [], [], []
        for g in range(n_chunk):
            h_g, kv_g = kv_project(parts[g], w_key, w_value, attn_gain, k_gain, cos_t, sin_t)
            hid.append(h_g)
            kv.append(kv_g)
            kv_all.append(lax.all_gather(kv_g, 'sp', axis=0, tiled=False))
        outs = []
        for g in range(n_chunk):
            q_g = jnp.dot(hid[g], w_query, preferred_element_type=jnp.float32).astype(jnp.bfloat16)
            o_g = attention(idx, q_g, kv_all[g], q_gain, cos_t, sin_t)
            proj = jnp.dot(o_g, w_out, preferred_element_type=jnp.float32)
            outs.append((parts[g].astype(jnp.float32) + proj).astype(jnp.bfloat16))
        out = jnp.concatenate(outs, axis=0).reshape(tokens.shape)
        kv_cat = jnp.concatenate(kv, axis=0)
        k_cache = kv_cat[:, :n_kv * HD].reshape(n_batch, seq_loc, n_kv, HD)
        v_cache = kv_cat[:, n_kv * HD:].reshape(n_batch, seq_loc, n_kv, HD)
        return out, k_cache, v_cache

    spec_tok = P('dp', 'sp', None)
    spec_cache = P('dp', 'sp', None, None)
    spec_mat = P(None, None)
    spec_vec = P(None)
    return jax.shard_map(per_device, mesh=mesh, in_specs=(spec_tok, spec_mat, spec_mat, spec_mat, spec_mat, spec_vec, spec_vec, spec_vec), out_specs=(spec_tok, spec_cache, spec_cache), check_vma=False)
```

```python
import functools

import jax
import jax.numpy as jnp
from jax import lax
from jax.experimental import pallas as pl
from jax.experimental.pallas import tpu as pltpu
from jax.sharding import PartitionSpec as P

EPS = 1e-6
THETA = 1000000.0
HD = 128
LOG2E = 1.4426950408889634
VMEM_LIMIT = 60 * 1024 * 1024
BLK = 256


def rope_tables(positions):
    half = HD // 2
    inv_freq = THETA ** (-jnp.arange(half, dtype=jnp.float32) * 2.0 / HD)
    angles = positions.astype(jnp.float32)[:, None] * inv_freq[None, :]
    cos_t, sin_t = jnp.cos(angles), jnp.sin(angles)
    return jnp.concatenate([cos_t, cos_t], axis=1), jnp.concatenate([-sin_t, sin_t], axis=1)


def head_norm_rope(raw, gain, cos_t, sin_t):
    inv = lax.rsqrt(jnp.mean(raw * raw, axis=-1, keepdims=True) + EPS)
    normed = raw * inv * gain
    return normed * cos_t + pltpu.roll(normed, HD // 2, 1) * sin_t


def kv_kernel(x_ref, g_ref, wk_ref, wv_ref, kg_ref, cos_ref, sin_ref, h_ref, kv_ref):
    wide = x_ref[...].astype(jnp.float32)
    inv = lax.rsqrt(jnp.mean(wide * wide, axis=-1, keepdims=True) + EPS)
    h_ref[...] = (wide * inv * g_ref[...]).astype(jnp.bfloat16)
    hid = h_ref[...]
    n_k = wk_ref.shape[1]
    step = 512
    for c in range(0, n_k, step):
        raw = jnp.dot(hid, wk_ref[:, c:c + step], preferred_element_type=jnp.float32)
        raw = raw.astype(jnp.bfloat16).astype(jnp.float32)
        for j in range(0, step, HD):
            k_rot = head_norm_rope(raw[:, j:j + HD], kg_ref[...], cos_ref[...], sin_ref[...])
            kv_ref[:, c + j:c + j + HD] = k_rot.astype(jnp.bfloat16)
    for c in range(0, n_k, step):
        raw = jnp.dot(hid, wv_ref[:, c:c + step], preferred_element_type=jnp.float32)
        kv_ref[:, n_k + c:n_k + c + step] = raw.astype(jnp.bfloat16)


def kv_project(x, first, n_blk, w_key, w_value, attn_gain, k_gain, cos_t, sin_t):
    d_model = x.shape[1]
    n_k = w_key.shape[1]
    rows = n_blk * BLK
    row_blk = lambda width: pl.BlockSpec((BLK, width), lambda i: (i, 0))
    full = lambda a: pl.BlockSpec(a.shape, lambda i: (0, 0), pipeline_mode=pl.Buffered(1))
    return pl.pallas_call(
        kv_kernel,
        grid=(n_blk,),
        in_specs=[pl.BlockSpec((BLK, d_model), lambda i: (first + i, 0))] + [full(a) for a in (attn_gain, w_key, w_value, k_gain, cos_t, sin_t)],
        out_specs=[row_blk(d_model), row_blk(2 * n_k)],
        out_shape=[jax.ShapeDtypeStruct((rows, d_model), jnp.bfloat16), jax.ShapeDtypeStruct((rows, 2 * n_k), jnp.bfloat16)],
        compiler_params=pltpu.CompilerParams(vmem_limit_bytes=VMEM_LIMIT, dimension_semantics=('arbitrary',)),
        cost_estimate=pl.CostEstimate(flops=4 * rows * d_model * n_k, bytes_accessed=rows * (d_model + n_k) * 4 + 4 * d_model * n_k, transcendentals=0),
        name='kv_project',
    )(x, attn_gain, w_key, w_value, k_gain, cos_t, sin_t)


def q_kernel(n_col, hid_ref, w_ref, qg_ref, cos_ref, sin_ref, q_ref, raw_s):
    i = pl.program_id(0)

    def dot(slot):
        raw_s[slot] = jnp.dot(hid_ref[...], w_ref[...], preferred_element_type=jnp.float32)

    def finish(slot):
        rows, width = q_ref.shape
        for r in range(0, rows, BLK):
            for c in range(0, width, HD):
                raw = raw_s[slot, r:r + BLK, c:c + HD].astype(jnp.bfloat16).astype(jnp.float32)
                q_ref[r:r + BLK, c:c + HD] = head_norm_rope(raw, qg_ref[...], cos_ref[...], sin_ref[...]).astype(jnp.bfloat16)

    @pl.when(i == 0)
    def _():
        dot(0)

    for slot in range(2):
        @pl.when(jnp.logical_and(jnp.logical_and(i > 0, i < n_col), i % 2 == slot))
        def _():
            dot(slot)
            finish(1 - slot)

    @pl.when(i == n_col)
    def _():
        finish((n_col - 1) % 2)


def q_project(hid, w_query, q_gain, cos_t, sin_t):
    rows, d_model = hid.shape
    bn = 512
    n_col = w_query.shape[1] // bn
    const = lambda a: pl.BlockSpec(a.shape, lambda i: (0, 0))
    return pl.pallas_call(
        functools.partial(q_kernel, n_col),
        grid=(n_col + 1,),
        in_specs=[pl.BlockSpec(hid.shape, lambda i: (0, 0), pipeline_mode=pl.Buffered(1)), pl.BlockSpec((d_model, bn), lambda i: (0, jnp.minimum(i, n_col - 1))), const(q_gain), const(cos_t), const(sin_t)],
        out_specs=pl.BlockSpec((rows, bn), lambda i: (0, jnp.maximum(i - 1, 0))),
        out_shape=jax.ShapeDtypeStruct((rows, w_query.shape[1]), jnp.bfloat16),
        scratch_shapes=[pltpu.VMEM((2, rows, bn), jnp.float32)],
        compiler_params=pltpu.CompilerParams(vmem_limit_bytes=VMEM_LIMIT, dimension_semantics=('arbitrary',)),
        cost_estimate=pl.CostEstimate(flops=2 * rows * w_query.size, bytes_accessed=2 * w_query.size + 4 * hid.size, transcendentals=0),
        name='q_project',
    )(hid, w_query, q_gain, cos_t, sin_t)


def out_kernel(o_ref, w_ref, x_ref, *rest):
    y_ref = rest[-1]
    y_ref[...] = (x_ref[...].astype(jnp.float32) + jnp.dot(o_ref[...], w_ref[...], preferred_element_type=jnp.float32)).astype(jnp.bfloat16)


def out_project(attn, w_out, x, g, so_far):
    rows, depth = attn.shape
    bn = 512
    tile = pl.BlockSpec((rows, bn), lambda i: (g, i))
    extra = [] if so_far is None else [so_far]
    return pl.pallas_call(
        out_kernel,
        grid=(w_out.shape[1] // bn,),
        in_specs=[pl.BlockSpec(attn.shape, lambda i: (0, 0), pipeline_mode=pl.Buffered(1)), pl.BlockSpec((depth, bn), lambda i: (0, i)), tile] + [pl.BlockSpec(memory_space=pl.ANY)] * len(extra),
        out_specs=tile,
        out_shape=jax.ShapeDtypeStruct(x.shape, jnp.bfloat16),
        input_output_aliases={3: 0} if extra else {},
        compiler_params=pltpu.CompilerParams(vmem_limit_bytes=VMEM_LIMIT, dimension_semantics=('arbitrary',)),
        cost_estimate=pl.CostEstimate(flops=2 * rows * w_out.size, bytes_accessed=2 * w_out.size + 6 * attn.size, transcendentals=0),
        name='out_project',
    )(attn, w_out, x, *extra)


def attn_kernel(n_group, n_head, blk, idx_ref, q_ref, k_ref, v_ref, o_ref, acc_s, m_s, l_s, s_s, p_s, a_s):
    last = idx_ref[0] // 2
    shift = (idx_ref[0] % 2) * blk
    scale = LOG2E * HD ** -0.5
    width = 2 * blk

    def load(ref, u, h):
        c = h // n_group * HD
        return ref[pl.ds(2 * u, 2), :, c:c + HD].reshape(width, HD)

    def qk(u, h):
        s_s[h % 2] = lax.dot_general(q_ref[:, h * HD:(h + 1) * HD], load(k_ref, u, h), (((1,), (1,)), ((), ())), preferred_element_type=jnp.float32)

    def fold(p):
        part = p[:, :HD]
        for j in range(HD, width, HD):
            part = part + p[:, j:j + HD]
        return part

    def soft(h, masked):
        s = s_s[h % 2]
        if masked:
            allowed = lax.broadcasted_iota(jnp.int32, s.shape, 1) <= lax.broadcasted_iota(jnp.int32, s.shape, 0) + shift
            s = jnp.where(allowed, s, -jnp.inf)
        m = jnp.broadcast_to(jnp.max(s, axis=1, keepdims=True) * scale, (blk, HD))
        if not masked:
            m_old = m_s[h]
            m = jnp.maximum(m_old, m)
            alpha = jnp.exp2(m_old - m)
            a_s[h % 2] = alpha
        p = jnp.exp2(s * scale - jnp.concatenate([m] * (width // HD), axis=1))
        m_s[h] = m
        l_s[h] = fold(p) if masked else l_s[h] * alpha + fold(p)
        p_s[h % 2] = p.astype(jnp.bfloat16)

    def pv(u, h, fresh):
        o = jnp.dot(p_s[h % 2], load(v_ref, u, h), preferred_element_type=jnp.float32)
        acc_s[h] = o if fresh else acc_s[h] * a_s[h % 2] + o

    end = n_head - 1
    qk(last, 0)
    for h in range(n_head):
        if h < end:
            qk(last, h + 1)
        else:
            qk(0, 0)
        if h > 0:
            pv(last, h - 1, True)
        soft(h, True)
    acc_s[end] = jnp.zeros_like(acc_s[end])
    a_s[end % 2] = jnp.zeros_like(a_s[end % 2])

    def body(u, _):
        for h in range(n_head):
            if h < end:
                qk(u, h + 1)
            else:
                qk(jnp.minimum(u + 1, last), 0)
            if h > 0:
                pv(u, h - 1, False)
            else:
                pv(jnp.where(u == 0, last, u - 1), end, False)
            soft(h, False)
        return 0

    lax.fori_loop(0, last, body, 0)
    pv(jnp.where(last == 0, 0, last - 1), end, False)
    for h in range(n_head):
        total = jnp.sum(l_s[h], axis=1, keepdims=True)
        o_ref[:, h * HD:(h + 1) * HD] = (acc_s[h] * (1.0 / total)).astype(jnp.bfloat16)

def attention(idx, q, kv_all, pair=2):
    n_dev, rows, kv_w = kv_all.shape
    n_kv = kv_w // (2 * HD)
    n_group = q.shape[1] // (n_kv * HD)
    n_head = pair * n_group
    blk = BLK
    qo = pl.BlockSpec((blk, n_head * HD), lambda b, h, i: (b, h))
    kv_spec = lambda off: pl.BlockSpec((n_dev, blk, pair * HD), lambda b, h, i: (0, b, off + h))
    f32 = lambda *shape: pltpu.VMEM(shape, jnp.float32)
    return pl.pallas_call(
        functools.partial(attn_kernel, n_group, n_head, blk),
        grid_spec=pltpu.PrefetchScalarGridSpec(
            num_scalar_prefetch=1,
            grid=(rows // blk, n_kv // pair),
            in_specs=[qo, kv_spec(0), kv_spec(n_kv // pair)],
            out_specs=qo,
            scratch_shapes=[f32(n_head, blk, HD)] * 3 + [f32(2, blk, 2 * blk), pltpu.VMEM((2, blk, 2 * blk), jnp.bfloat16), f32(2, blk, HD)],
        ),
        out_shape=jax.ShapeDtypeStruct(q.shape, jnp.bfloat16),
        compiler_params=pltpu.CompilerParams(vmem_limit_bytes=VMEM_LIMIT, dimension_semantics=('arbitrary', 'arbitrary')),
        cost_estimate=pl.CostEstimate(flops=8 * rows * q.shape[1] * n_dev * blk, bytes_accessed=4 * q.size + 2 * kv_all.size, transcendentals=0),
        name='attention',
    )(idx, q, kv_all, kv_all)


def solution(mesh):
    def per_device(tokens, w_query, w_key, w_value, w_out, attn_norm, q_norm, k_norm):
        n_batch, seq_loc, d_model = tokens.shape
        me = lax.axis_index('sp')
        cos_t, sin_t = rope_tables(me * seq_loc + jnp.arange(seq_loc))
        attn_gain = attn_norm.astype(jnp.float32)[None, :]
        q_gain = q_norm.astype(jnp.float32)[None, :]
        k_gain = k_norm.astype(jnp.float32)[None, :]
        idx = jnp.reshape(me, (1,)).astype(jnp.int32)
        flat = tokens.reshape(n_batch * seq_loc, d_model)
        n_kv = w_key.shape[1] // HD

        n_chunk = 4
        n_blk = n_batch // n_chunk
        hid, kv, kv_all = [], [], []
        for g in range(n_chunk):
            h_g, kv_g = kv_project(flat, g * n_blk, n_blk, w_key, w_value, attn_gain, k_gain, cos_t, sin_t)
            hid.append(h_g)
            kv.append(kv_g)
            kv_all.append(lax.all_gather(kv_g, 'sp', axis=0, tiled=False))
        out = None
        for g in range(n_chunk):
            q_g = q_project(hid[g], w_query, q_gain, cos_t, sin_t)
            out = out_project(attention(idx, q_g, kv_all[g]), w_out, flat, g, out)
        out = out.reshape(tokens.shape)
        kv_cat = jnp.concatenate(kv, axis=0)
        k_cache = kv_cat[:, :n_kv * HD].reshape(n_batch, seq_loc, n_kv, HD)
        v_cache = kv_cat[:, n_kv * HD:].reshape(n_batch, seq_loc, n_kv, HD)
        return out, k_cache, v_cache

    spec_tok = P('dp', 'sp', None)
    spec_cache = P('dp', 'sp', None, None)
    spec_mat = P(None, None)
    spec_vec = P(None)
    return jax.shard_map(per_device, mesh=mesh, in_specs=(spec_tok, spec_mat, spec_mat, spec_mat, spec_mat, spec_vec, spec_vec, spec_vec), out_specs=(spec_tok, spec_cache, spec_cache), check_vma=False)
```

```python
import functools

import jax
import jax.numpy as jnp
from jax import lax
from jax.experimental import pallas as pl
from jax.experimental.pallas import tpu as pltpu
from jax.sharding import PartitionSpec as P

EPS = 1e-6
THETA = 1000000.0
HD = 128
LOG2E = 1.4426950408889634
VMEM_LIMIT = 60 * 1024 * 1024
BLK = 256
PLAN = ('heads', 'heads', 'keys', 'keys')


def rope_tables(positions):
    half = HD // 2
    inv_freq = THETA ** (-jnp.arange(half, dtype=jnp.float32) * 2.0 / HD)
    angles = positions.astype(jnp.float32)[:, None] * inv_freq[None, :]
    cos_t, sin_t = jnp.cos(angles), jnp.sin(angles)
    return jnp.concatenate([cos_t, cos_t], axis=1), jnp.concatenate([-sin_t, sin_t], axis=1)


def head_norm_rope(raw, gain, cos_t, sin_t):
    inv = lax.rsqrt(jnp.mean(raw * raw, axis=-1, keepdims=True) + EPS)
    normed = raw * inv * gain
    return normed * cos_t + pltpu.roll(normed, HD // 2, 1) * sin_t


def kv_kernel(x_ref, g_ref, wk_ref, wv_ref, kg_ref, cos_ref, sin_ref, h_ref, kv_ref):
    rows, n_k = x_ref.shape[0], wk_ref.shape[1]
    for r in range(0, rows, 128):
        wide = x_ref[r:r + 128].astype(jnp.float32)
        inv = lax.rsqrt(jnp.mean(wide * wide, axis=-1, keepdims=True) + EPS)
        h_ref[r:r + 128] = (wide * inv * g_ref[...]).astype(jnp.bfloat16)
    step = 512
    for c in range(0, n_k, step):
        raw = jnp.dot(h_ref[...], wk_ref[:, c:c + step], preferred_element_type=jnp.float32).astype(jnp.bfloat16)
        for j in range(0, step, HD):
            for r in range(0, rows, BLK):
                k_rot = head_norm_rope(raw[r:r + BLK, j:j + HD].astype(jnp.float32), kg_ref[...], cos_ref[...], sin_ref[...])
                kv_ref[(c + j) // HD, r:r + BLK, :HD] = k_rot.astype(jnp.bfloat16)
    for c in range(0, n_k, step):
        raw = jnp.dot(h_ref[...], wv_ref[:, c:c + step], preferred_element_type=jnp.float32).astype(jnp.bfloat16)
        for j in range(0, step, HD):
            kv_ref[(c + j) // HD, :, HD:] = raw[:, j:j + HD]


def kv_project(x, first, n_prompt, w_key, w_value, attn_gain, k_gain, cos_t, sin_t):
    d_model = x.shape[1]
    n_k = w_key.shape[1]
    rows = n_prompt * BLK
    bm = 2 * BLK if n_prompt % 2 == 0 and first % 2 == 0 else BLK
    off = first * BLK // bm
    full = lambda a: pl.BlockSpec(a.shape, lambda i: (0, 0), pipeline_mode=pl.Buffered(1))
    return pl.pallas_call(
        kv_kernel,
        grid=(rows // bm,),
        in_specs=[pl.BlockSpec((bm, d_model), lambda i: (off + i, 0))] + [full(a) for a in (attn_gain, w_key, w_value, k_gain, cos_t, sin_t)],
        out_specs=[pl.BlockSpec((bm, d_model), lambda i: (i, 0)), pl.BlockSpec((n_k // HD, bm, 2 * HD), lambda i: (0, i, 0))],
        out_shape=[jax.ShapeDtypeStruct((rows, d_model), jnp.bfloat16), jax.ShapeDtypeStruct((n_k // HD, rows, 2 * HD), jnp.bfloat16)],
        compiler_params=pltpu.CompilerParams(vmem_limit_bytes=VMEM_LIMIT, dimension_semantics=('arbitrary',)),
        cost_estimate=pl.CostEstimate(flops=4 * rows * d_model * n_k, bytes_accessed=rows * (d_model + n_k) * 4 + 4 * d_model * n_k, transcendentals=0),
        name='kv_project',
    )(x, attn_gain, w_key, w_value, k_gain, cos_t, sin_t)


def q_kernel(n_col, hid_ref, w_ref, qg_ref, cos_ref, sin_ref, q_ref, raw_s):
    i = pl.program_id(0)

    def dot(slot):
        raw_s[slot] = jnp.dot(hid_ref[...], w_ref[...], preferred_element_type=jnp.float32)

    def finish(slot):
        rows, width = q_ref.shape
        for r in range(0, rows, BLK):
            for c in range(0, width, HD):
                raw = raw_s[slot, r:r + BLK, c:c + HD].astype(jnp.bfloat16).astype(jnp.float32)
                q_ref[r:r + BLK, c:c + HD] = head_norm_rope(raw, qg_ref[...], cos_ref[...], sin_ref[...]).astype(jnp.bfloat16)

    @pl.when(i == 0)
    def _():
        dot(0)

    for slot in range(2):
        @pl.when(jnp.logical_and(jnp.logical_and(i > 0, i < n_col), i % 2 == slot))
        def _():
            dot(slot)
            finish(1 - slot)

    @pl.when(i == n_col)
    def _():
        finish((n_col - 1) % 2)


def q_project(hid, n_kv, w_query, q_gain, cos_t, sin_t):
    rows, d_model = hid.shape
    bn = w_query.shape[1] // n_kv
    n_col = w_query.shape[1] // bn
    const = lambda a: pl.BlockSpec(a.shape, lambda i: (0, 0))
    return pl.pallas_call(
        functools.partial(q_kernel, n_col),
        grid=(n_col + 1,),
        in_specs=[pl.BlockSpec(hid.shape, lambda i: (0, 0), pipeline_mode=pl.Buffered(1)), pl.BlockSpec((d_model, bn), lambda i: (0, jnp.minimum(i, n_col - 1))), const(q_gain), const(cos_t), const(sin_t)],
        out_specs=pl.BlockSpec((None, rows, bn), lambda i: (jnp.maximum(i - 1, 0), 0, 0)),
        out_shape=jax.ShapeDtypeStruct((n_col, rows, bn), jnp.bfloat16),
        scratch_shapes=[pltpu.VMEM((2, rows, bn), jnp.float32)],
        compiler_params=pltpu.CompilerParams(vmem_limit_bytes=VMEM_LIMIT, dimension_semantics=('arbitrary',)),
        cost_estimate=pl.CostEstimate(flops=2 * rows * w_query.size, bytes_accessed=2 * w_query.size + 4 * hid.size, transcendentals=0),
        name='q_project',
    )(hid, w_query, q_gain, cos_t, sin_t)


def out_kernel(o_ref, w_ref, x_ref, *rest):
    y_ref, flat_s, sem = rest[-3:]
    width = o_ref.shape[2]

    @pl.when(pl.program_id(0) == 0)
    def _():
        copies = [pltpu.make_async_copy(o_ref.at[h], flat_s.at[:, h * width:(h + 1) * width], sem.at[h]) for h in range(o_ref.shape[0])]
        for copy in copies:
            copy.start()
        for copy in copies:
            copy.wait()

    y_ref[...] = (x_ref[...].astype(jnp.float32) + jnp.dot(flat_s[...], w_ref[...], preferred_element_type=jnp.float32)).astype(jnp.bfloat16)


def out_project(attn, w_out, x, first, so_far):
    n_kv, rows, width = attn.shape
    depth = n_kv * width
    bn = 512
    g = first * BLK // rows
    tile = pl.BlockSpec((rows, bn), lambda i: (g, i))
    extra = [] if so_far is None else [so_far]
    anywhere = pl.BlockSpec(memory_space=pl.ANY)
    return pl.pallas_call(
        out_kernel,
        grid=(w_out.shape[1] // bn,),
        in_specs=[anywhere, pl.BlockSpec((depth, bn), lambda i: (0, i)), tile] + [anywhere] * len(extra),
        out_specs=tile,
        out_shape=jax.ShapeDtypeStruct(x.shape, jnp.bfloat16),
        input_output_aliases={3: 0} if extra else {},
        scratch_shapes=[pltpu.VMEM((rows, depth), jnp.bfloat16), pltpu.SemaphoreType.DMA((n_kv,))],
        compiler_params=pltpu.CompilerParams(vmem_limit_bytes=VMEM_LIMIT, dimension_semantics=('arbitrary',)),
        cost_estimate=pl.CostEstimate(flops=2 * rows * w_out.size, bytes_accessed=2 * w_out.size + 6 * attn.size, transcendentals=0),
        name='out_project',
    )(attn, w_out, x, *extra)


def attn_kernel(by_head, n_group, idx_ref, q_ref, k_ref, v_ref, o_ref, acc_s, m_s, l_s, s_s, p_s, a_s):
    piece = pl.program_id(1) if by_head else idx_ref[0]
    blk = q_ref.shape[1]
    n_head = q_ref.shape[0] * n_group
    last = piece // 2
    shift = (piece % 2) * blk
    scale = LOG2E * HD ** -0.5
    width = 2 * blk

    def load(ref, u, h):
        return ref[pl.ds(2 * u, 2), h // n_group].reshape(width, HD)

    def cols(h):
        return h // n_group, slice(None), slice(h % n_group * HD, (h % n_group + 1) * HD)

    def qk(u, h):
        s_s[h % 2] = lax.dot_general(q_ref[cols(h)], load(k_ref, u, h), (((1,), (1,)), ((), ())), preferred_element_type=jnp.float32)

    def fold(p):
        part = p[:, :HD]
        for j in range(HD, width, HD):
            part = part + p[:, j:j + HD]
        return part

    def soft(h, masked):
        s = s_s[h % 2]
        if masked:
            allowed = lax.broadcasted_iota(jnp.int32, s.shape, 1) <= lax.broadcasted_iota(jnp.int32, s.shape, 0) + shift
            s = jnp.where(allowed, s, -jnp.inf)
        m = jnp.broadcast_to(jnp.max(s, axis=1, keepdims=True) * scale, (blk, HD))
        if not masked:
            m_old = m_s[h]
            m = jnp.maximum(m_old, m)
            alpha = jnp.exp2(m_old - m)
            a_s[h % 2] = alpha
        p = jnp.exp2(s * scale - jnp.concatenate([m] * (width // HD), axis=1))
        m_s[h] = m
        l_s[h] = fold(p) if masked else l_s[h] * alpha + fold(p)
        p_s[h % 2] = p.astype(jnp.bfloat16)

    def pv(u, h, fresh):
        o = jnp.dot(p_s[h % 2], load(v_ref, u, h), preferred_element_type=jnp.float32)
        acc_s[h] = o if fresh else acc_s[h] * a_s[h % 2] + o

    end = n_head - 1
    qk(last, 0)
    for h in range(n_head):
        if h < end:
            qk(last, h + 1)
        else:
            qk(0, 0)
        if h > 0:
            pv(last, h - 1, True)
        soft(h, True)
    acc_s[end] = jnp.zeros_like(acc_s[end])
    a_s[end % 2] = jnp.zeros_like(a_s[end % 2])

    def body(u, _):
        for h in range(n_head):
            if h < end:
                qk(u, h + 1)
            else:
                qk(jnp.minimum(u + 1, last), 0)
            if h > 0:
                pv(u, h - 1, False)
            else:
                pv(jnp.where(u == 0, last, u - 1), end, False)
            soft(h, False)
        return 0

    lax.fori_loop(0, last, body, 0)
    pv(jnp.where(last == 0, 0, last - 1), end, False)
    for h in range(n_head):
        total = jnp.sum(l_s[h], axis=1, keepdims=True)
        o_ref[cols(h)] = (acc_s[h] * (1.0 / total)).astype(jnp.bfloat16)

def attention(idx, q, kv, by_head):
    n_piece, n_kv, rows, _ = kv.shape
    n_slab, _, width = q.shape
    n_group = width // HD
    pair = 1 if by_head else 2
    n_head = pair * n_group
    qo = pl.BlockSpec((pair, BLK, width), lambda b, h, i: (h, b, 0))
    kv_spec = lambda half: pl.BlockSpec((n_piece, pair, BLK, HD), lambda b, h, i: (0, 0 if by_head else h, b, half))
    f32 = lambda *shape: pltpu.VMEM(shape, jnp.float32)
    work = 5 if by_head else n_piece
    return pl.pallas_call(
        functools.partial(attn_kernel, by_head, n_group),
        grid_spec=pltpu.PrefetchScalarGridSpec(
            num_scalar_prefetch=1,
            grid=(rows // BLK, n_slab // pair),
            in_specs=[qo, kv_spec(0), kv_spec(1)],
            out_specs=qo,
            scratch_shapes=[f32(n_head, BLK, HD)] * 3 + [f32(2, BLK, 2 * BLK), pltpu.VMEM((2, BLK, 2 * BLK), jnp.bfloat16), f32(2, BLK, HD)],
        ),
        out_shape=jax.ShapeDtypeStruct(q.shape, jnp.bfloat16),
        compiler_params=pltpu.CompilerParams(vmem_limit_bytes=VMEM_LIMIT, dimension_semantics=('arbitrary', 'arbitrary')),
        cost_estimate=pl.CostEstimate(flops=8 * q.size * work * BLK, bytes_accessed=4 * q.size + 2 * kv.size, transcendentals=0),
        name='attention',
    )(idx, q, kv, kv)


def solution(mesh):
    def per_device(tokens, w_query, w_key, w_value, w_out, attn_norm, q_norm, k_norm):
        n_batch, seq_loc, d_model = tokens.shape
        me = lax.axis_index('sp')
        cos_t, sin_t = rope_tables(me * seq_loc + jnp.arange(seq_loc))
        attn_gain = attn_norm.astype(jnp.float32)[None, :]
        q_gain = q_norm.astype(jnp.float32)[None, :]
        k_gain = k_norm.astype(jnp.float32)[None, :]
        idx = jnp.reshape(me, (1,)).astype(jnp.int32)
        flat = tokens.reshape(n_batch * seq_loc, d_model)
        n_kv = w_key.shape[1] // HD

        n_chunk = len(PLAN)
        n_prompt = n_batch // n_chunk
        order = sorted(range(n_chunk), key=lambda g: PLAN[g] != 'heads')
        swap = lambda a: lax.all_to_all(a, 'sp', 0, 0, tiled=True)
        q, kv, moved, mixed = {}, {}, {}, {}
        hid = {}
        for g in order:
            hid[g], kv[g] = kv_project(flat, g * n_prompt, n_prompt, w_key, w_value, attn_gain, k_gain, cos_t, sin_t)
            if PLAN[g] == 'heads':
                moved[g] = swap(kv[g])[:, None]
                q[g] = swap(q_project(hid[g], n_kv, w_query, q_gain, cos_t, sin_t))
            else:
                moved[g] = lax.all_gather(kv[g], 'sp', axis=0, tiled=False)
        for g in order:
            if PLAN[g] == 'heads':
                mixed[g] = swap(attention(idx, q[g], moved[g], True))
            else:
                mixed[g] = attention(idx, q_project(hid[g], n_kv, w_query, q_gain, cos_t, sin_t), moved[g], False)
        out = None
        for g in reversed(order):
            out = out_project(mixed[g], w_out, flat, g * n_prompt, out)
        out = out.reshape(tokens.shape)

        def cache(half):
            parts = [jnp.swapaxes(kv[g][:, :, half * HD:(half + 1) * HD], 0, 1) for g in range(n_chunk)]
            return jnp.concatenate(parts, axis=0).reshape(n_batch, seq_loc, n_kv, HD)

        k_cache, v_cache = cache(0), cache(1)
        return out, k_cache, v_cache

    spec_tok = P('dp', 'sp', None)
    spec_cache = P('dp', 'sp', None, None)
    spec_mat = P(None, None)
    spec_vec = P(None)
    return jax.shard_map(per_device, mesh=mesh, in_specs=(spec_tok, spec_mat, spec_mat, spec_mat, spec_mat, spec_vec, spec_vec, spec_vec), out_specs=(spec_tok, spec_cache, spec_cache), check_vma=False)
```

```python
import functools

import jax
import jax.numpy as jnp
from jax import lax
from jax.experimental import pallas as pl
from jax.experimental.pallas import tpu as pltpu
from jax.sharding import PartitionSpec as P

EPS = 1e-6
THETA = 1000000.0
HD = 128
LOG2E = 1.4426950408889634
VMEM_LIMIT = 60 * 1024 * 1024
BLK = 256


def rope_tables(positions):
    half = HD // 2
    inv_freq = THETA ** (-jnp.arange(half, dtype=jnp.float32) * 2.0 / HD)
    angles = positions.astype(jnp.float32)[:, None] * inv_freq[None, :]
    cos_t, sin_t = jnp.cos(angles), jnp.sin(angles)
    return jnp.concatenate([cos_t, cos_t], axis=1), jnp.concatenate([-sin_t, sin_t], axis=1)


def head_norm_rope(raw, gain, cos_t, sin_t):
    inv = lax.rsqrt(jnp.mean(raw * raw, axis=-1, keepdims=True) + EPS)
    normed = raw * inv * gain
    return normed * cos_t + pltpu.roll(normed, HD // 2, 1) * sin_t


def kv_kernel(x_ref, g_ref, wk_ref, wv_ref, kg_ref, cos_ref, sin_ref, h_ref, kv_ref):
    wide = x_ref[...].astype(jnp.float32)
    inv = lax.rsqrt(jnp.mean(wide * wide, axis=-1, keepdims=True) + EPS)
    h_ref[...] = (wide * inv * g_ref[...]).astype(jnp.bfloat16)
    hid = h_ref[...]
    n_k = wk_ref.shape[1]
    step = 512
    for c in range(0, n_k, step):
        raw = jnp.dot(hid, wk_ref[:, c:c + step], preferred_element_type=jnp.float32)
        raw = raw.astype(jnp.bfloat16).astype(jnp.float32)
        for j in range(0, step, HD):
            k_rot = head_norm_rope(raw[:, j:j + HD], kg_ref[...], cos_ref[...], sin_ref[...])
            kv_ref[:, c + j:c + j + HD] = k_rot.astype(jnp.bfloat16)
    for c in range(0, n_k, step):
        raw = jnp.dot(hid, wv_ref[:, c:c + step], preferred_element_type=jnp.float32)
        kv_ref[:, n_k + c:n_k + c + step] = raw.astype(jnp.bfloat16)


def kv_project(x, first, n_blk, w_key, w_value, attn_gain, k_gain, cos_t, sin_t):
    d_model = x.shape[1]
    n_k = w_key.shape[1]
    rows = n_blk * BLK
    row_blk = lambda width: pl.BlockSpec((BLK, width), lambda i: (i, 0))
    full = lambda a: pl.BlockSpec(a.shape, lambda i: (0, 0), pipeline_mode=pl.Buffered(1))
    return pl.pallas_call(
        kv_kernel,
        grid=(n_blk,),
        in_specs=[pl.BlockSpec((BLK, d_model), lambda i: (first + i, 0))] + [full(a) for a in (attn_gain, w_key, w_value, k_gain, cos_t, sin_t)],
        out_specs=[row_blk(d_model), row_blk(2 * n_k)],
        out_shape=[jax.ShapeDtypeStruct((rows, d_model), jnp.bfloat16), jax.ShapeDtypeStruct((rows, 2 * n_k), jnp.bfloat16)],
        compiler_params=pltpu.CompilerParams(vmem_limit_bytes=VMEM_LIMIT, dimension_semantics=('arbitrary',)),
        cost_estimate=pl.CostEstimate(flops=4 * rows * d_model * n_k, bytes_accessed=rows * (d_model + n_k) * 4 + 4 * d_model * n_k, transcendentals=0),
        name='kv_project',
    )(x, attn_gain, w_key, w_value, k_gain, cos_t, sin_t)


def q_kernel(n_col, hid_ref, w_ref, qg_ref, cos_ref, sin_ref, q_ref, raw_s):
    i = pl.program_id(0)

    def dot(slot):
        raw_s[slot] = jnp.dot(hid_ref[...], w_ref[...], preferred_element_type=jnp.float32)

    def finish(slot):
        rows, width = q_ref.shape
        for r in range(0, rows, BLK):
            for c in range(0, width, HD):
                raw = raw_s[slot, r:r + BLK, c:c + HD].astype(jnp.bfloat16).astype(jnp.float32)
                q_ref[r:r + BLK, c:c + HD] = head_norm_rope(raw, qg_ref[...], cos_ref[...], sin_ref[...]).astype(jnp.bfloat16)

    @pl.when(i == 0)
    def _():
        dot(0)

    for slot in range(2):
        @pl.when(jnp.logical_and(jnp.logical_and(i > 0, i < n_col), i % 2 == slot))
        def _():
            dot(slot)
            finish(1 - slot)

    @pl.when(i == n_col)
    def _():
        finish((n_col - 1) % 2)


def q_project(hid, w_query, q_gain, cos_t, sin_t):
    rows, d_model = hid.shape
    bn = 512
    n_col = w_query.shape[1] // bn
    const = lambda a: pl.BlockSpec(a.shape, lambda i: (0, 0))
    return pl.pallas_call(
        functools.partial(q_kernel, n_col),
        grid=(n_col + 1,),
        in_specs=[pl.BlockSpec(hid.shape, lambda i: (0, 0), pipeline_mode=pl.Buffered(1)), pl.BlockSpec((d_model, bn), lambda i: (0, jnp.minimum(i, n_col - 1))), const(q_gain), const(cos_t), const(sin_t)],
        out_specs=pl.BlockSpec((rows, bn), lambda i: (0, jnp.maximum(i - 1, 0))),
        out_shape=jax.ShapeDtypeStruct((rows, w_query.shape[1]), jnp.bfloat16),
        scratch_shapes=[pltpu.VMEM((2, rows, bn), jnp.float32)],
        compiler_params=pltpu.CompilerParams(vmem_limit_bytes=VMEM_LIMIT, dimension_semantics=('arbitrary',)),
        cost_estimate=pl.CostEstimate(flops=2 * rows * w_query.size, bytes_accessed=2 * w_query.size + 4 * hid.size, transcendentals=0),
        name='q_project',
    )(hid, w_query, q_gain, cos_t, sin_t)


def out_kernel(o_ref, w_ref, x_ref, *rest):
    y_ref = rest[-1]
    y_ref[...] = (x_ref[...].astype(jnp.float32) + jnp.dot(o_ref[...], w_ref[...], preferred_element_type=jnp.float32)).astype(jnp.bfloat16)


def out_project(attn, w_out, x, g, so_far):
    rows, depth = attn.shape
    bn = 512
    tile = pl.BlockSpec((rows, bn), lambda i: (g, i))
    extra = [] if so_far is None else [so_far]
    return pl.pallas_call(
        out_kernel,
        grid=(w_out.shape[1] // bn,),
        in_specs=[pl.BlockSpec(attn.shape, lambda i: (0, 0), pipeline_mode=pl.Buffered(1)), pl.BlockSpec((depth, bn), lambda i: (0, i)), tile] + [pl.BlockSpec(memory_space=pl.ANY)] * len(extra),
        out_specs=tile,
        out_shape=jax.ShapeDtypeStruct(x.shape, jnp.bfloat16),
        input_output_aliases={3: 0} if extra else {},
        compiler_params=pltpu.CompilerParams(vmem_limit_bytes=VMEM_LIMIT, dimension_semantics=('arbitrary',)),
        cost_estimate=pl.CostEstimate(flops=2 * rows * w_out.size, bytes_accessed=2 * w_out.size + 6 * attn.size, transcendentals=0),
        name='out_project',
    )(attn, w_out, x, *extra)


def attn_kernel(pair, n_group, idx_ref, q_ref, *rest):
    k_refs, v_refs = rest[:pair], rest[pair:2 * pair]
    o_ref, acc_s, m_s, l_s, a_s, s_s, p_s, vt_s = rest[2 * pair:]
    n_head = pair * n_group
    blk = q_ref.shape[0]
    width = 2 * blk
    last = idx_ref[0] // 2
    shift = (idx_ref[0] % 2) * blk
    scale = LOG2E * HD ** -0.5

    def load(ref, u):
        return ref[pl.ds(2 * u, 2)].reshape(width, HD)

    def turn(u, slot):
        for c in range(pair):
            vt_s[slot, c] = load(v_refs[c], u).T

    def score(u, h, diag):
        q = q_ref[:, h * HD:(h + 1) * HD]
        s = lax.dot_general(load(k_refs[h // n_group], u), q, (((1,), (1,)), ((), ())), preferred_element_type=jnp.float32)
        if diag:
            allowed = lax.broadcasted_iota(jnp.int32, s.shape, 0) <= lax.broadcasted_iota(jnp.int32, s.shape, 1) + shift
            s = jnp.where(allowed, s, -jnp.inf)
        s_s[h % 2] = s
        m = jnp.max(s, axis=0, keepdims=True) * scale
        if not diag:
            m_old = m_s[h]
            m = jnp.maximum(m_old, m)
            a_s[h] = jnp.exp2(m_old - m)
        m_s[h] = m

    def soft(h, diag):
        p = jnp.exp2(s_s[h % 2] * scale - m_s[h])
        part = jnp.sum(p, axis=0, keepdims=True)
        l_s[h] = part if diag else l_s[h] * a_s[h] + part
        p_s[h % 2] = p.astype(jnp.bfloat16)

    def gather_v(slot, h, diag):
        o = jnp.dot(vt_s[slot, h // n_group], p_s[h % 2], preferred_element_type=jnp.float32)
        acc_s[h] = o if diag else acc_s[h] * a_s[h] + o

    end = n_head - 1
    turn(last, 0)
    score(last, 0, True)
    for h in range(n_head):
        if h < end:
            score(last, h + 1, True)
        else:
            score(0, 0, False)
        if h > 0:
            gather_v(0, h - 1, True)
        soft(h, True)
    acc_s[end] = jnp.zeros_like(acc_s[end])
    a_s[end] = jnp.zeros_like(a_s[end])

    def body(u, _):
        turn(u, (u + 1) % 2)
        for h in range(n_head):
            if h < end:
                score(u, h + 1, False)
            else:
                score(jnp.minimum(u + 1, last), 0, False)
            if h > 0:
                gather_v((u + 1) % 2, h - 1, False)
            else:
                gather_v(u % 2, end, False)
            soft(h, False)
        return 0

    lax.fori_loop(0, last, body, 0)
    gather_v(last % 2, end, False)
    for h in range(n_head):
        o_ref[:, h * HD:(h + 1) * HD] = (acc_s[h] * (1.0 / l_s[h])).T.astype(jnp.bfloat16)


def attention(idx, q, kv_all, pair=2):
    n_dev, rows, kv_w = kv_all.shape
    n_kv = kv_w // (2 * HD)
    n_group = q.shape[1] // (n_kv * HD)
    n_head = pair * n_group
    qo = pl.BlockSpec((BLK, n_head * HD), lambda b, h, i: (b, h))
    head_spec = lambda c: pl.BlockSpec((n_dev, BLK, HD), lambda b, h, i: (0, b, pair * h + c))
    vm = lambda *shape, dtype=jnp.float32: pltpu.VMEM(shape, dtype)
    return pl.pallas_call(
        functools.partial(attn_kernel, pair, n_group),
        grid_spec=pltpu.PrefetchScalarGridSpec(
            num_scalar_prefetch=1,
            grid=(rows // BLK, n_kv // pair),
            in_specs=[qo] + [head_spec(c) for c in range(pair)] + [head_spec(n_kv + c) for c in range(pair)],
            out_specs=qo,
            scratch_shapes=[vm(n_head, HD, BLK)] + [vm(n_head, 1, BLK)] * 3 + [vm(2, 2 * BLK, BLK), vm(2, 2 * BLK, BLK, dtype=jnp.bfloat16), vm(2, pair, HD, 2 * BLK, dtype=jnp.bfloat16)],
        ),
        out_shape=jax.ShapeDtypeStruct(q.shape, jnp.bfloat16),
        compiler_params=pltpu.CompilerParams(vmem_limit_bytes=VMEM_LIMIT, dimension_semantics=('arbitrary', 'arbitrary')),
        cost_estimate=pl.CostEstimate(flops=8 * rows * q.shape[1] * n_dev * BLK, bytes_accessed=4 * q.size + 2 * kv_all.size, transcendentals=0),
        name='attention',
    )(idx, q, *([kv_all] * (2 * pair)))


def solution(mesh):
    def per_device(tokens, w_query, w_key, w_value, w_out, attn_norm, q_norm, k_norm):
        n_batch, seq_loc, d_model = tokens.shape
        me = lax.axis_index('sp')
        cos_t, sin_t = rope_tables(me * seq_loc + jnp.arange(seq_loc))
        attn_gain = attn_norm.astype(jnp.float32)[None, :]
        q_gain = q_norm.astype(jnp.float32)[None, :]
        k_gain = k_norm.astype(jnp.float32)[None, :]
        idx = jnp.reshape(me, (1,)).astype(jnp.int32)
        flat = tokens.reshape(n_batch * seq_loc, d_model)
        n_kv = w_key.shape[1] // HD

        n_chunk = 4
        n_blk = n_batch // n_chunk
        hid, kv, kv_all = [], [], []
        for g in range(n_chunk):
            h_g, kv_g = kv_project(flat, g * n_blk, n_blk, w_key, w_value, attn_gain, k_gain, cos_t, sin_t)
            hid.append(h_g)
            kv.append(kv_g)
            kv_all.append(lax.all_gather(kv_g, 'sp', axis=0, tiled=False))
        out = None
        for g in range(n_chunk):
            q_g = q_project(hid[g], w_query, q_gain, cos_t, sin_t)
            out = out_project(attention(idx, q_g, kv_all[g]), w_out, flat, g, out)
        out = out.reshape(tokens.shape)
        kv_cat = jnp.concatenate(kv, axis=0)
        k_cache = kv_cat[:, :n_kv * HD].reshape(n_batch, seq_loc, n_kv, HD)
        v_cache = kv_cat[:, n_kv * HD:].reshape(n_batch, seq_loc, n_kv, HD)
        return out, k_cache, v_cache

    spec_tok = P('dp', 'sp', None)
    spec_cache = P('dp', 'sp', None, None)
    spec_mat = P(None, None)
    spec_vec = P(None)
    return jax.shard_map(per_device, mesh=mesh, in_specs=(spec_tok, spec_mat, spec_mat, spec_mat, spec_mat, spec_vec, spec_vec, spec_vec), out_specs=(spec_tok, spec_cache, spec_cache), check_vma=False)
```

```python
import functools

import jax
import jax.numpy as jnp
from jax import lax
from jax.experimental import pallas as pl
from jax.experimental.pallas import tpu as pltpu
from jax.sharding import PartitionSpec as P

EPS = 1e-6
THETA = 1000000.0
HD = 128
LOG2E = 1.4426950408889634
VMEM_LIMIT = 60 * 1024 * 1024
BLK = 256


def rope_tables(positions):
    half = HD // 2
    inv_freq = THETA ** (-jnp.arange(half, dtype=jnp.float32) * 2.0 / HD)
    angles = positions.astype(jnp.float32)[:, None] * inv_freq[None, :]
    cos_t, sin_t = jnp.cos(angles), jnp.sin(angles)
    return jnp.concatenate([cos_t, cos_t], axis=1), jnp.concatenate([-sin_t, sin_t], axis=1)


def head_norm_rope(raw, gain, cos_t, sin_t):
    inv = lax.rsqrt(jnp.mean(raw * raw, axis=-1, keepdims=True) + EPS)
    normed = raw * inv * gain
    return normed * cos_t + pltpu.roll(normed, HD // 2, 1) * sin_t


def kv_kernel(sizes, x_ref, g_ref, wk_ref, wv_ref, kg_ref, cos_ref, sin_ref, h_ref, *rest):
    kv_refs, kv_s = rest[:-1], rest[-1]
    wide = x_ref[...].astype(jnp.float32)
    inv = lax.rsqrt(jnp.mean(wide * wide, axis=-1, keepdims=True) + EPS)
    h_ref[...] = (wide * inv * g_ref[...]).astype(jnp.bfloat16)
    hid = h_ref[...]
    n_k = wk_ref.shape[1]
    step = 512
    for c in range(0, n_k, step):
        raw = jnp.dot(hid, wk_ref[:, c:c + step], preferred_element_type=jnp.float32)
        raw = raw.astype(jnp.bfloat16).astype(jnp.float32)
        for j in range(0, step, HD):
            k_rot = head_norm_rope(raw[:, j:j + HD], kg_ref[...], cos_ref[...], sin_ref[...])
            kv_s[:, c + j:c + j + HD] = k_rot.astype(jnp.bfloat16)
    for c in range(0, n_k, step):
        raw = jnp.dot(hid, wv_ref[:, c:c + step], preferred_element_type=jnp.float32)
        kv_s[:, n_k + c:n_k + c + step] = raw.astype(jnp.bfloat16)
    i, start = pl.program_id(0), 0
    for ref, size in zip(kv_refs, sizes):
        @pl.when(jnp.logical_and(i >= start, i < start + size))
        def _():
            ref[...] = kv_s[...]
        start += size


def kv_project(x, first, sizes, w_key, w_value, attn_gain, k_gain, cos_t, sin_t):
    d_model = x.shape[1]
    n_k = w_key.shape[1]
    rows = sum(sizes) * BLK
    full = lambda a: pl.BlockSpec(a.shape, lambda i: (0, 0), pipeline_mode=pl.Buffered(1))
    part = lambda start, size: pl.BlockSpec((BLK, 2 * n_k), lambda i: (jnp.clip(i - start, 0, size - 1), 0))
    starts = [sum(sizes[:c]) for c in range(len(sizes))]
    hid, *kvs = pl.pallas_call(
        functools.partial(kv_kernel, sizes),
        grid=(sum(sizes),),
        in_specs=[pl.BlockSpec((BLK, d_model), lambda i: (first + i, 0))] + [full(a) for a in (attn_gain, w_key, w_value, k_gain, cos_t, sin_t)],
        out_specs=[pl.BlockSpec((BLK, d_model), lambda i: (i, 0))] + [part(*a) for a in zip(starts, sizes)],
        out_shape=[jax.ShapeDtypeStruct((rows, d_model), jnp.bfloat16)] + [jax.ShapeDtypeStruct((size * BLK, 2 * n_k), jnp.bfloat16) for size in sizes],
        scratch_shapes=[pltpu.VMEM((BLK, 2 * n_k), jnp.bfloat16)],
        compiler_params=pltpu.CompilerParams(vmem_limit_bytes=VMEM_LIMIT, dimension_semantics=('arbitrary',)),
        cost_estimate=pl.CostEstimate(flops=4 * rows * d_model * n_k, bytes_accessed=rows * (d_model + n_k) * 4 + 4 * d_model * n_k, transcendentals=0),
        name='kv_project',
    )(x, attn_gain, w_key, w_value, k_gain, cos_t, sin_t)
    return hid, kvs


def q_kernel(n_col, hid_ref, w_ref, qg_ref, cos_ref, sin_ref, q_ref, raw_s):
    i = pl.program_id(0)

    def dot(slot):
        raw_s[slot] = jnp.dot(hid_ref[...], w_ref[...], preferred_element_type=jnp.float32)

    def finish(slot):
        rows, width = q_ref.shape
        for r in range(0, rows, BLK):
            for c in range(0, width, HD):
                raw = raw_s[slot, r:r + BLK, c:c + HD].astype(jnp.bfloat16).astype(jnp.float32)
                q_ref[r:r + BLK, c:c + HD] = head_norm_rope(raw, qg_ref[...], cos_ref[...], sin_ref[...]).astype(jnp.bfloat16)

    @pl.when(i < n_col)
    def _():
        dot(i % 2)
        finish((i + 1) % 2)

    @pl.when(i == n_col)
    def _():
        finish((n_col - 1) % 2)


def q_project(hid, first, n_prompt, w_query, q_gain, cos_t, sin_t):
    rows, d_model = n_prompt * BLK, hid.shape[1]
    g = first * BLK // rows
    bn = 512
    n_col = w_query.shape[1] // bn
    const = lambda a: pl.BlockSpec(a.shape, lambda i: (0, 0))
    return pl.pallas_call(
        functools.partial(q_kernel, n_col),
        grid=(n_col + 1,),
        in_specs=[pl.BlockSpec((rows, d_model), lambda i: (g, 0), pipeline_mode=pl.Buffered(1)), pl.BlockSpec((d_model, bn), lambda i: (0, jnp.minimum(i, n_col - 1))), const(q_gain), const(cos_t), const(sin_t)],
        out_specs=pl.BlockSpec((rows, bn), lambda i: (0, jnp.maximum(i - 1, 0))),
        out_shape=jax.ShapeDtypeStruct((rows, w_query.shape[1]), jnp.bfloat16),
        scratch_shapes=[pltpu.VMEM((2, rows, bn), jnp.float32)],
        compiler_params=pltpu.CompilerParams(vmem_limit_bytes=VMEM_LIMIT, dimension_semantics=('arbitrary',)),
        cost_estimate=pl.CostEstimate(flops=2 * rows * w_query.size, bytes_accessed=2 * w_query.size + 4 * rows * d_model, transcendentals=0),
        name='q_project',
    )(hid, w_query, q_gain, cos_t, sin_t)


def out_kernel(o_ref, w_ref, x_ref, *rest):
    y_ref = rest[-1]
    y_ref[...] = (x_ref[...].astype(jnp.float32) + jnp.dot(o_ref[...], w_ref[...], preferred_element_type=jnp.float32)).astype(jnp.bfloat16)


def out_project(attn, w_out, x, g, so_far):
    rows, depth = attn.shape
    bn = 512
    tile = pl.BlockSpec((rows, bn), lambda i: (g, i))
    extra = [] if so_far is None else [so_far]
    return pl.pallas_call(
        out_kernel,
        grid=(w_out.shape[1] // bn,),
        in_specs=[pl.BlockSpec(attn.shape, lambda i: (0, 0), pipeline_mode=pl.Buffered(1)), pl.BlockSpec((depth, bn), lambda i: (0, i)), tile] + [pl.BlockSpec(memory_space=pl.ANY)] * len(extra),
        out_specs=tile,
        out_shape=jax.ShapeDtypeStruct(x.shape, jnp.bfloat16),
        input_output_aliases={3: 0} if extra else {},
        compiler_params=pltpu.CompilerParams(vmem_limit_bytes=VMEM_LIMIT, dimension_semantics=('arbitrary',)),
        cost_estimate=pl.CostEstimate(flops=2 * rows * w_out.size, bytes_accessed=2 * w_out.size + 6 * attn.size, transcendentals=0),
        name='out_project',
    )(attn, w_out, x, *extra)


def pick_kernel(idx_ref, own_ref, other_ref, w_ref, x_ref, so_far_ref, y_ref, attn_s, sem):
    @pl.when(pl.program_id(0) == 0)
    def _():
        for here, ref in ((1, own_ref), (0, other_ref)):
            @pl.when(idx_ref[1] == here)
            def _():
                copy = pltpu.make_async_copy(ref, attn_s, sem)
                copy.start()
                copy.wait()

    out_kernel(attn_s, w_ref, x_ref, y_ref)


def out_project_pick(idx, own, other, w_out, x, first, so_far):
    rows, depth = own.shape
    bn = 512
    g = first * BLK // rows
    tile = pl.BlockSpec((rows, bn), lambda i, s: (g, i))
    anywhere = pl.BlockSpec(memory_space=pl.ANY)
    return pl.pallas_call(
        pick_kernel,
        grid_spec=pltpu.PrefetchScalarGridSpec(
            num_scalar_prefetch=1,
            grid=(w_out.shape[1] // bn,),
            in_specs=[anywhere, anywhere, pl.BlockSpec((depth, bn), lambda i, s: (0, i)), tile, anywhere],
            out_specs=tile,
            scratch_shapes=[pltpu.VMEM((rows, depth), jnp.bfloat16), pltpu.SemaphoreType.DMA],
        ),
        out_shape=jax.ShapeDtypeStruct(x.shape, jnp.bfloat16),
        input_output_aliases={5: 0},
        compiler_params=pltpu.CompilerParams(vmem_limit_bytes=VMEM_LIMIT, dimension_semantics=('arbitrary',)),
        cost_estimate=pl.CostEstimate(flops=2 * rows * w_out.size, bytes_accessed=2 * w_out.size + 6 * own.size, transcendentals=0),
        name='out_project',
    )(idx, own, other, w_out, x, so_far)


def attn_kernel(pair, n_group, idx_ref, q_ref, *rest):
    k_refs, v_refs = rest[:pair], rest[pair:2 * pair]
    o_ref, acc_s, m_s, l_s, a_s, s_s, p_s, vt_s = rest[2 * pair:]
    n_head = pair * n_group
    blk = q_ref.shape[0]
    width = 2 * blk
    last = idx_ref[0] // 2
    shift = (idx_ref[0] % 2) * blk
    scale = LOG2E * HD ** -0.5

    def load(ref, u):
        return ref[pl.ds(2 * u, 2)].reshape(width, HD)

    def turn(u, slot):
        for c in range(pair):
            vt_s[slot, c] = load(v_refs[c], u).T

    def score(u, h, diag):
        q = q_ref[:, h * HD:(h + 1) * HD]
        s = lax.dot_general(load(k_refs[h // n_group], u), q, (((1,), (1,)), ((), ())), preferred_element_type=jnp.float32)
        if diag:
            allowed = lax.broadcasted_iota(jnp.int32, s.shape, 0) <= lax.broadcasted_iota(jnp.int32, s.shape, 1) + shift
            s = jnp.where(allowed, s, -jnp.inf)
        s_s[h % 2] = s
        m = jnp.max(s, axis=0, keepdims=True) * scale
        if not diag:
            m_old = m_s[h]
            m = jnp.maximum(m_old, m)
            a_s[h] = jnp.exp2(m_old - m)
        m_s[h] = m

    def soft(h, diag):
        p = jnp.exp2(s_s[h % 2] * scale - m_s[h])
        part = jnp.sum(p, axis=0, keepdims=True)
        l_s[h] = part if diag else l_s[h] * a_s[h] + part
        p_s[h % 2] = p.astype(jnp.bfloat16)

    def gather_v(slot, h, diag):
        o = jnp.dot(vt_s[slot, h // n_group], p_s[h % 2], preferred_element_type=jnp.float32)
        acc_s[h] = o if diag else acc_s[h] * a_s[h] + o

    @pl.when(idx_ref[1] == 1)
    def _():
        end = n_head - 1
        turn(last, 0)
        score(last, 0, True)
        for h in range(n_head):
            if h < end:
                score(last, h + 1, True)
            else:
                score(0, 0, False)
            if h > 0:
                gather_v(0, h - 1, True)
            soft(h, True)
        acc_s[end] = jnp.zeros_like(acc_s[end])
        a_s[end] = jnp.zeros_like(a_s[end])

        def body(u, _):
            turn(u, (u + 1) % 2)
            for h in range(n_head):
                if h < end:
                    score(u, h + 1, False)
                else:
                    score(jnp.minimum(u + 1, last), 0, False)
                if h > 0:
                    gather_v((u + 1) % 2, h - 1, False)
                else:
                    gather_v(u % 2, end, False)
                soft(h, False)
            return 0

        lax.fori_loop(0, last, body, 0)
        gather_v(last % 2, end, False)
        for h in range(n_head):
            o_ref[:, h * HD:(h + 1) * HD] = (acc_s[h] * (1.0 / l_s[h])).T.astype(jnp.bfloat16)


def attention(idx, q, kv_all, pair=2):
    n_dev, rows, kv_w = kv_all.shape
    n_kv = kv_w // (2 * HD)
    n_group = q.shape[1] // (n_kv * HD)
    n_head = pair * n_group
    qo = pl.BlockSpec((BLK, n_head * HD), lambda b, h, i: (b * i[1], h * i[1]))
    head_spec = lambda c: pl.BlockSpec((n_dev, BLK, HD), lambda b, h, i: (0, b * i[1], (pair * h) * i[1] + c))
    vm = lambda *shape, dtype=jnp.float32: pltpu.VMEM(shape, dtype)
    return pl.pallas_call(
        functools.partial(attn_kernel, pair, n_group),
        grid_spec=pltpu.PrefetchScalarGridSpec(
            num_scalar_prefetch=1,
            grid=(rows // BLK, n_kv // pair),
            in_specs=[qo] + [head_spec(c) for c in range(pair)] + [head_spec(n_kv + c) for c in range(pair)],
            out_specs=qo,
            scratch_shapes=[vm(n_head, HD, BLK)] + [vm(n_head, 1, BLK)] * 3 + [vm(2, 2 * BLK, BLK), vm(2, 2 * BLK, BLK, dtype=jnp.bfloat16), vm(2, pair, HD, 2 * BLK, dtype=jnp.bfloat16)],
        ),
        out_shape=jax.ShapeDtypeStruct(q.shape, jnp.bfloat16),
        compiler_params=pltpu.CompilerParams(vmem_limit_bytes=VMEM_LIMIT, dimension_semantics=('arbitrary', 'arbitrary')),
        cost_estimate=pl.CostEstimate(flops=8 * rows * q.shape[1] * n_dev * BLK, bytes_accessed=4 * q.size + 2 * kv_all.size, transcendentals=0),
        name='attention',
    )(idx, q, *([kv_all] * (2 * pair)))


def solution(mesh):
    def per_device(tokens, w_query, w_key, w_value, w_out, attn_norm, q_norm, k_norm):
        n_batch, seq_loc, d_model = tokens.shape
        me = lax.axis_index('sp')
        cos_t, sin_t = rope_tables(me * seq_loc + jnp.arange(seq_loc))
        attn_gain = attn_norm.astype(jnp.float32)[None, :]
        q_gain = q_norm.astype(jnp.float32)[None, :]
        k_gain = k_norm.astype(jnp.float32)[None, :]
        n_dev = mesh.shape['sp']
        pieces = lambda piece, active: jnp.stack([piece, active]).astype(jnp.int32)
        always, early = jnp.ones_like(me), (me < n_dev // 2).astype(me.dtype)
        flat = tokens.reshape(n_batch * seq_loc, d_model)
        n_kv = w_key.shape[1] // HD

        n_far = n_batch // 8
        sizes = tuple([2 * n_far] * 3 + [n_far])
        starts = [sum(sizes[:c]) for c in range(len(sizes))]
        far = sum(sizes)
        gather = lambda a: lax.all_gather(a, 'sp', axis=0, tiled=False)
        kv_args = (w_key, w_value, attn_gain, k_gain, cos_t, sin_t)
        q_args = (w_query, q_gain, cos_t, sin_t)

        hid_far, (kv_far,) = kv_project(flat, far, (n_far,), *kv_args)
        all_far = gather(kv_far)
        q_far = q_project(hid_far, 0, n_far, *q_args)
        q_got = lax.ppermute(q_far, 'sp', [(d, n_dev - 1 - d) for d in range(n_dev // 2, n_dev)])
        flat_main, q_far = lax.optimization_barrier((flat, q_far))
        hid, kv = kv_project(flat_main, 0, sizes, *kv_args)
        kv_all = [gather(a) for a in kv]
        o_got = attention(pieces(n_dev - 1 - me, early), q_got, all_far)
        o_back = lax.ppermute(o_got, 'sp', [(d, n_dev - 1 - d) for d in range(n_dev // 2)])
        o_far = attention(pieces(me, early), q_far, all_far)
        out = None
        for c, n in enumerate(sizes):
            q_c = q_project(hid, starts[c], n, *q_args)
            if out is not None:
                q_c, out = lax.optimization_barrier((q_c, out))
            out = out_project(attention(pieces(me, always), q_c, kv_all[c]), w_out, flat, starts[c] // n, out)
        out = out_project_pick(pieces(me, early), o_far, o_back, w_out, flat, far, out)
        out = out.reshape(tokens.shape)
        kv_cat = jnp.concatenate(kv + [kv_far], axis=0)
        k_cache = kv_cat[:, :n_kv * HD].reshape(n_batch, seq_loc, n_kv, HD)
        v_cache = kv_cat[:, n_kv * HD:].reshape(n_batch, seq_loc, n_kv, HD)
        return out, k_cache, v_cache

    spec_tok = P('dp', 'sp', None)
    spec_cache = P('dp', 'sp', None, None)
    spec_mat = P(None, None)
    spec_vec = P(None)
    return jax.shard_map(per_device, mesh=mesh, in_specs=(spec_tok, spec_mat, spec_mat, spec_mat, spec_mat, spec_vec, spec_vec, spec_vec), out_specs=(spec_tok, spec_cache, spec_cache), check_vma=False)
```

```python
import functools

import jax
import jax.numpy as jnp
from jax import lax
from jax.experimental import pallas as pl
from jax.experimental.pallas import tpu as pltpu
from jax.sharding import PartitionSpec as P

EPS = 1e-6
THETA = 1000000.0
HD = 128
LOG2E = 1.4426950408889634
VMEM_LIMIT = 60 * 1024 * 1024
BLK = 256


def rope_tables(positions):
    half = HD // 2
    inv_freq = THETA ** (-jnp.arange(half, dtype=jnp.float32) * 2.0 / HD)
    angles = positions.astype(jnp.float32)[:, None] * inv_freq[None, :]
    cos_t, sin_t = jnp.cos(angles), jnp.sin(angles)
    return jnp.concatenate([cos_t, cos_t], axis=1), jnp.concatenate([-sin_t, sin_t], axis=1)


def head_norm_rope(raw, gain, cos_t, sin_t):
    inv = lax.rsqrt(jnp.mean(raw * raw, axis=-1, keepdims=True) + EPS)
    normed = raw * inv * gain
    return normed * cos_t + pltpu.roll(normed, HD // 2, 1) * sin_t


def kv_kernel(sizes, x_ref, g_ref, wk_ref, wv_ref, kg_ref, cos_ref, sin_ref, h_ref, *rest):
    kv_refs, kv_s = rest[:-1], rest[-1]
    wide = x_ref[...].astype(jnp.float32)
    inv = lax.rsqrt(jnp.mean(wide * wide, axis=-1, keepdims=True) + EPS)
    h_ref[...] = (wide * inv * g_ref[...]).astype(jnp.bfloat16)
    hid = h_ref[...]
    n_k = wk_ref.shape[1]
    step = 512
    for c in range(0, n_k, step):
        raw = jnp.dot(hid, wk_ref[:, c:c + step], preferred_element_type=jnp.float32)
        raw = raw.astype(jnp.bfloat16).astype(jnp.float32)
        for j in range(0, step, HD):
            k_rot = head_norm_rope(raw[:, j:j + HD], kg_ref[...], cos_ref[...], sin_ref[...])
            kv_s[:, c + j:c + j + HD] = k_rot.astype(jnp.bfloat16)
    for c in range(0, n_k, step):
        raw = jnp.dot(hid, wv_ref[:, c:c + step], preferred_element_type=jnp.float32)
        kv_s[:, n_k + c:n_k + c + step] = raw.astype(jnp.bfloat16)
    i, start = pl.program_id(0), 0
    for ref, size in zip(kv_refs, sizes):
        @pl.when(jnp.logical_and(i >= start, i < start + size))
        def _():
            ref[...] = kv_s[...]
        start += size


def kv_project(x, first, sizes, w_key, w_value, attn_gain, k_gain, cos_t, sin_t):
    d_model = x.shape[1]
    n_k = w_key.shape[1]
    rows = sum(sizes) * BLK
    full = lambda a: pl.BlockSpec(a.shape, lambda i: (0, 0), pipeline_mode=pl.Buffered(1))
    part = lambda start, size: pl.BlockSpec((BLK, 2 * n_k), lambda i: (jnp.clip(i - start, 0, size - 1), 0))
    starts = [sum(sizes[:c]) for c in range(len(sizes))]
    hid, *kvs = pl.pallas_call(
        functools.partial(kv_kernel, sizes),
        grid=(sum(sizes),),
        in_specs=[pl.BlockSpec((BLK, d_model), lambda i: (first + i, 0))] + [full(a) for a in (attn_gain, w_key, w_value, k_gain, cos_t, sin_t)],
        out_specs=[pl.BlockSpec((BLK, d_model), lambda i: (i, 0))] + [part(*a) for a in zip(starts, sizes)],
        out_shape=[jax.ShapeDtypeStruct((rows, d_model), jnp.bfloat16)] + [jax.ShapeDtypeStruct((size * BLK, 2 * n_k), jnp.bfloat16) for size in sizes],
        scratch_shapes=[pltpu.VMEM((BLK, 2 * n_k), jnp.bfloat16)],
        compiler_params=pltpu.CompilerParams(vmem_limit_bytes=VMEM_LIMIT, dimension_semantics=('arbitrary',)),
        cost_estimate=pl.CostEstimate(flops=4 * rows * d_model * n_k, bytes_accessed=rows * (d_model + n_k) * 4 + 4 * d_model * n_k, transcendentals=0),
        name='kv_project',
    )(x, attn_gain, w_key, w_value, k_gain, cos_t, sin_t)
    return hid, kvs


def q_kernel(n_step, hid_ref, w_ref, qg_ref, cos_ref, sin_ref, q_ref, raw_s):
    i = pl.program_id(0)

    def finish(slot):
        rows, width = q_ref.shape
        for r in range(0, rows, BLK):
            for c in range(0, width, HD):
                raw = raw_s[slot, r:r + BLK, c:c + HD].astype(jnp.bfloat16).astype(jnp.float32)
                q_ref[r:r + BLK, c:c + HD] = head_norm_rope(raw, qg_ref[...], cos_ref[...], sin_ref[...]).astype(jnp.bfloat16)

    for slot in range(2):
        @pl.when(jnp.logical_and(i < n_step, i % 2 == slot))
        def _():
            raw_s[slot] = jnp.dot(hid_ref[...], w_ref[...], preferred_element_type=jnp.float32)
            finish(1 - slot)

    @pl.when(i == n_step)
    def _():
        finish((n_step - 1) % 2)


def q_project(hid, n_prompt, w_query, q_gain, cos_t, sin_t):
    rows, d_model = hid.shape
    bm, bn = n_prompt * BLK, 512
    n_col = w_query.shape[1] // bn
    n_step = rows // bm * n_col
    const = lambda a: pl.BlockSpec(a.shape, lambda i: (0, 0))
    now = lambda i: jnp.minimum(i, n_step - 1)
    ago = lambda i: jnp.maximum(i - 1, 0)
    return pl.pallas_call(
        functools.partial(q_kernel, n_step),
        grid=(n_step + 1,),
        in_specs=[pl.BlockSpec((bm, d_model), lambda i: (now(i) // n_col, 0)), pl.BlockSpec((d_model, bn), lambda i: (0, now(i) % n_col)), const(q_gain), const(cos_t), const(sin_t)],
        out_specs=pl.BlockSpec((bm, bn), lambda i: (ago(i) // n_col, ago(i) % n_col)),
        out_shape=jax.ShapeDtypeStruct((rows, w_query.shape[1]), jnp.bfloat16),
        scratch_shapes=[pltpu.VMEM((2, bm, bn), jnp.float32)],
        compiler_params=pltpu.CompilerParams(vmem_limit_bytes=VMEM_LIMIT, dimension_semantics=('arbitrary',)),
        cost_estimate=pl.CostEstimate(flops=2 * rows * w_query.size, bytes_accessed=2 * w_query.size * (rows // bm) + 4 * rows * d_model, transcendentals=0),
        name='q_project',
    )(hid, w_query, q_gain, cos_t, sin_t)


def out_kernel(o_ref, w_ref, x_ref, *rest):
    y_ref = rest[-1]
    y_ref[...] = (x_ref[...].astype(jnp.float32) + jnp.dot(o_ref[...], w_ref[...], preferred_element_type=jnp.float32)).astype(jnp.bfloat16)


def out_project(attn, w_out, x, g, so_far):
    rows, depth = attn.shape
    bn = 512
    tile = pl.BlockSpec((rows, bn), lambda i: (g, i))
    extra = [] if so_far is None else [so_far]
    return pl.pallas_call(
        out_kernel,
        grid=(w_out.shape[1] // bn,),
        in_specs=[pl.BlockSpec(attn.shape, lambda i: (0, 0), pipeline_mode=pl.Buffered(1)), pl.BlockSpec((depth, bn), lambda i: (0, i)), tile] + [pl.BlockSpec(memory_space=pl.ANY)] * len(extra),
        out_specs=tile,
        out_shape=jax.ShapeDtypeStruct(x.shape, jnp.bfloat16),
        input_output_aliases={3: 0} if extra else {},
        compiler_params=pltpu.CompilerParams(vmem_limit_bytes=VMEM_LIMIT, dimension_semantics=('arbitrary',)),
        cost_estimate=pl.CostEstimate(flops=2 * rows * w_out.size, bytes_accessed=2 * w_out.size + 6 * attn.size, transcendentals=0),
        name='out_project',
    )(attn, w_out, x, *extra)


def attn_kernel(pair, n_group, idx_ref, q_ref, *rest):
    k_refs, v_refs = rest[:pair], rest[pair:2 * pair]
    o_ref, acc_s, m_s, l_s, a_s, s_s, p_s, vt_s = rest[2 * pair:]
    n_head = pair * n_group
    blk = q_ref.shape[0]
    width = 2 * blk
    last = idx_ref[0] // 2
    shift = (idx_ref[0] % 2) * blk
    scale = LOG2E * HD ** -0.5

    def load(ref, u):
        return ref[pl.ds(2 * u, 2)].reshape(width, HD)

    def turn(u, slot):
        for c in range(pair):
            vt_s[slot, c] = load(v_refs[c], u).T

    def score(u, h, diag):
        q = q_ref[:, h * HD:(h + 1) * HD]
        s = lax.dot_general(load(k_refs[h // n_group], u), q, (((1,), (1,)), ((), ())), preferred_element_type=jnp.float32)
        if diag:
            allowed = lax.broadcasted_iota(jnp.int32, s.shape, 0) <= lax.broadcasted_iota(jnp.int32, s.shape, 1) + shift
            s = jnp.where(allowed, s, -jnp.inf)
        s_s[h % 2] = s
        m = jnp.max(s, axis=0, keepdims=True) * scale
        if not diag:
            m_old = m_s[h]
            m = jnp.maximum(m_old, m)
            a_s[h] = jnp.exp2(m_old - m)
        m_s[h] = m

    def soft(h, diag):
        p = jnp.exp2(s_s[h % 2] * scale - m_s[h])
        part = jnp.sum(p, axis=0, keepdims=True)
        l_s[h] = part if diag else l_s[h] * a_s[h] + part
        p_s[h % 2] = p.astype(jnp.bfloat16)

    def gather_v(slot, h, diag):
        o = jnp.dot(vt_s[slot, h // n_group], p_s[h % 2], preferred_element_type=jnp.float32)
        acc_s[h] = o if diag else acc_s[h] * a_s[h] + o

    end = n_head - 1
    turn(last, 0)
    score(last, 0, True)
    for h in range(n_head):
        if h < end:
            score(last, h + 1, True)
        else:
            score(0, 0, False)
        if h > 0:
            gather_v(0, h - 1, True)
        soft(h, True)
    acc_s[end] = jnp.zeros_like(acc_s[end])
    a_s[end] = jnp.zeros_like(a_s[end])

    def body(u, _):
        turn(u, (u + 1) % 2)
        for h in range(n_head):
            if h < end:
                score(u, h + 1, False)
            else:
                score(jnp.minimum(u + 1, last), 0, False)
            if h > 0:
                gather_v((u + 1) % 2, h - 1, False)
            else:
                gather_v(u % 2, end, False)
            soft(h, False)
        return 0

    lax.fori_loop(0, last, body, 0)
    gather_v(last % 2, end, False)
    for h in range(n_head):
        o_ref[:, h * HD:(h + 1) * HD] = (acc_s[h] * (1.0 / l_s[h])).T.astype(jnp.bfloat16)


def attention(idx, q, first, kv_all, pair=2):
    n_dev, rows, kv_w = kv_all.shape
    n_kv = kv_w // (2 * HD)
    n_group = q.shape[1] // (n_kv * HD)
    n_head = pair * n_group
    tile = lambda off: pl.BlockSpec((BLK, n_head * HD), lambda b, h, i: (off + b, h))
    head_spec = lambda c: pl.BlockSpec((n_dev, BLK, HD), lambda b, h, i: (0, b, pair * h + c))
    vm = lambda *shape, dtype=jnp.float32: pltpu.VMEM(shape, dtype)
    return pl.pallas_call(
        functools.partial(attn_kernel, pair, n_group),
        grid_spec=pltpu.PrefetchScalarGridSpec(
            num_scalar_prefetch=1,
            grid=(rows // BLK, n_kv // pair),
            in_specs=[tile(first)] + [head_spec(c) for c in range(pair)] + [head_spec(n_kv + c) for c in range(pair)],
            out_specs=tile(0),
            scratch_shapes=[vm(n_head, HD, BLK)] + [vm(n_head, 1, BLK)] * 3 + [vm(2, 2 * BLK, BLK), vm(2, 2 * BLK, BLK, dtype=jnp.bfloat16), vm(2, pair, HD, 2 * BLK, dtype=jnp.bfloat16)],
        ),
        out_shape=jax.ShapeDtypeStruct((rows, q.shape[1]), jnp.bfloat16),
        compiler_params=pltpu.CompilerParams(vmem_limit_bytes=VMEM_LIMIT, dimension_semantics=('arbitrary', 'arbitrary')),
        cost_estimate=pl.CostEstimate(flops=8 * rows * q.shape[1] * n_dev * BLK, bytes_accessed=4 * rows * q.shape[1] + 2 * kv_all.size, transcendentals=0),
        name='attention',
    )(idx, q, *([kv_all] * (2 * pair)))


def solution(mesh):
    def per_device(tokens, w_query, w_key, w_value, w_out, attn_norm, q_norm, k_norm):
        n_batch, seq_loc, d_model = tokens.shape
        me = lax.axis_index('sp')
        cos_t, sin_t = rope_tables(me * seq_loc + jnp.arange(seq_loc))
        attn_gain = attn_norm.astype(jnp.float32)[None, :]
        q_gain = q_norm.astype(jnp.float32)[None, :]
        k_gain = k_norm.astype(jnp.float32)[None, :]
        idx = jnp.reshape(me, (1,)).astype(jnp.int32)
        flat = tokens.reshape(n_batch * seq_loc, d_model)
        n_kv = w_key.shape[1] // HD

        n_chunk = 4
        n = n_batch // n_chunk
        kv_args = (w_key, w_value, attn_gain, k_gain, cos_t, sin_t)
        q_args = (n, w_query, q_gain, cos_t, sin_t)
        hid_0, kv_0 = kv_project(flat, 0, (n,), *kv_args)
        hid_1, kv_1 = kv_project(flat, n, (n,) * (n_chunk - 1), *kv_args)
        kv = kv_0 + kv_1
        kv_all = [lax.all_gather(a, 'sp', axis=0, tiled=False) for a in kv]
        q_0, q_1 = q_project(hid_0, *q_args), q_project(hid_1, *q_args)
        out = None
        for g in range(n_chunk):
            q, first = (q_0, 0) if g == 0 else (q_1, (g - 1) * n)
            if out is not None:
                idx, out = lax.optimization_barrier((idx, out))
            out = out_project(attention(idx, q, first, kv_all[g]), w_out, flat, g, out)
        out = out.reshape(tokens.shape)
        kv_cat = jnp.concatenate(kv, axis=0)
        k_cache = kv_cat[:, :n_kv * HD].reshape(n_batch, seq_loc, n_kv, HD)
        v_cache = kv_cat[:, n_kv * HD:].reshape(n_batch, seq_loc, n_kv, HD)
        return out, k_cache, v_cache

    spec_tok = P('dp', 'sp', None)
    spec_cache = P('dp', 'sp', None, None)
    spec_mat = P(None, None)
    spec_vec = P(None)
    return jax.shard_map(per_device, mesh=mesh, in_specs=(spec_tok, spec_mat, spec_mat, spec_mat, spec_mat, spec_vec, spec_vec, spec_vec), out_specs=(spec_tok, spec_cache, spec_cache), check_vma=False)
```
